32 devices in a mesh: row: 4 (over z), col: 8 (over y, x, core).
Axes of the slice: x: 2, y: 2, z: 4, core: 2. Of those that a mesh axis runs over, the one named last changes fastest.
Arguments:
- shallow_state: float32 [128, 2, 128, 128], P('col'), may hold values from -6 to 6
- shallow_prev: float32 [128, 2, 128, 128], P('col'), may hold values from -6 to 6
- deep_state: float32 [576, 2, 128, 128], P(('row', 'col')), may hold values from -6 to 6
- deep_prev: float32 [576, 2, 128, 128], P(('row', 'col')), may hold values from -6 to 6
- hamilton: float32 [128, 128], replicated, as said below
- couple: float32 [14, 128, 128], replicated, as said below
- gamma: float32 [14], replicated, may hold values from 0.2 to 5
- coef_real: float32 [14], replicated, may hold values from 0.2 to 2
- coef_imag: float32 [14], replicated, may hold values from 0.1 to 1
- shallow_bath: int32 [128, 2], P('col'), may hold values from -1 to 13, as said below
- shallow_lower: int32 [128, 2], P('col'), may hold values from -1 to 127, as said below
- deep_bath: int32 [576, 3], P(('row', 'col')), may hold values from -1 to 13, as said below
- deep_lower: int32 [576, 3], P(('row', 'col')), may hold values from -1 to 127, as said below
Outputs:
- shallow_slope: float32 [128, 2, 128, 128], P('col')
- deep_slope: float32 [576, 2, 128, 128], P(('row', 'col'))
The draws below stay inside these ranges and needn't reach their ends.
Inputs may be any that keep to these rules, and one draw needn't show every extreme that they name: `shallow_bath`: A live slot of tier t lists t baths in non-decreasing order followed by -1; every multi-index of tier 0, 1 or 2 over 14 baths stands in exactly one of the 128 slots; the other slots hold only -1. `shallow_lower`: entry u is the slot holding the multi-index with unit u removed, and -1 exactly where the unit is -1. `deep_bath`: A live slot lists 3 baths in non-decreasing order; every multi-index of tier 3 over 14 baths stands in exactly one of the 576 slots; the other slots hold only -1. `deep_lower`: entry u is the shallow slot holding the multi-index with unit u removed, and -1 exactly where the unit is -1. `hamilton`: Symmetric. `couple`: each operator symmetric.
All inputs are finite; a program needn't handle non-finite values.
Results may differ from the reference program's by a relative error of at most 0.0001.
Values sent between devices are 32-bit elements; how exact they have to be, the bound alone decides.
No kernel may reach another device: no remote copies, remote signals or barrier semaphores. Data moves between devices by JAX's collectives and lax.ppermute only.
A program may use at most 192 MiB of HBM per device.

```python
import math
import jax
import jax.numpy as jnp
import numpy as np
from jax import lax

N = 128
K = 14
SHALLOW = 120
DEEP = 560
SH_TOTAL = 128
DEEP_TOTAL = 576


def hierarchy_tables(bath_count):
    shallow_list = [()] + [(first,) for first in range(bath_count)]
    shallow_list = shallow_list + [(first, second) for first in range(bath_count) for second in range(first, bath_count)]
    deep_list = [(first, second, third) for first in range(bath_count) for second in range(first, bath_count) for third in range(second, bath_count)]
    position_map = {}
    for position, entries in enumerate(shallow_list):
        position_map[entries] = position
    shallow_units = np.full((len(shallow_list), 2), -1, np.int32)
    shallow_below = np.full((len(shallow_list), 2), -1, np.int32)
    for position, entries in enumerate(shallow_list):
        for column in range(len(entries)):
            shallow_units[position, column] = entries[column]
            shallow_below[position, column] = position_map[entries[:column] + entries[column + 1:]]
    deep_units = np.full((len(deep_list), 3), -1, np.int32)
    deep_below = np.full((len(deep_list), 3), -1, np.int32)
    for position, entries in enumerate(deep_list):
        for column in range(3):
            deep_units[position, column] = entries[column]
            deep_below[position, column] = position_map[entries[:column] + entries[column + 1:]]
    return (shallow_units, shallow_below, deep_units, deep_below)


def layout_tables(key):
    shallow_units, shallow_below, deep_units, deep_below = hierarchy_tables(K)
    shallow_slots = jax.random.permutation(jax.random.fold_in(key, 11), SH_TOTAL)[:SHALLOW].astype(jnp.int32)
    deep_slots = jax.random.permutation(jax.random.fold_in(key, 13), DEEP_TOTAL)[:DEEP].astype(jnp.int32)
    units_in = jnp.asarray(shallow_units)
    below_ids = jnp.asarray(shallow_below)
    below_in = jnp.where(below_ids >= 0, shallow_slots[jnp.maximum(below_ids, 0)], -1)
    shallow_bath = jnp.full((SH_TOTAL, 2), -1, jnp.int32).at[shallow_slots].set(units_in)
    shallow_lower = jnp.full((SH_TOTAL, 2), -1, jnp.int32).at[shallow_slots].set(below_in)
    deep_ids = jnp.asarray(deep_below)
    deep_in = shallow_slots[deep_ids]
    deep_bath = jnp.full((DEEP_TOTAL, 3), -1, jnp.int32).at[deep_slots].set(jnp.asarray(deep_units))
    deep_lower = jnp.full((DEEP_TOTAL, 3), -1, jnp.int32).at[deep_slots].set(deep_in)
    return (shallow_bath, shallow_lower, deep_bath, deep_lower)


def draw_shallow_bath(key, part):
    return layout_tables(key)[0]


def draw_shallow_lower(key, part):
    return layout_tables(key)[1]


def draw_deep_bath(key, part):
    return layout_tables(key)[2]


def draw_deep_lower(key, part):
    return layout_tables(key)[3]


def draw_hamilton(key, part):
    base = jax.random.normal(jax.random.fold_in(key, 21), (N, N), jnp.float32) / math.sqrt(2.0 * N)
    energy = jax.random.uniform(jax.random.fold_in(key, 22), (N,), jnp.float32, -1.0, 1.0)
    return base + base.T + jnp.diag(energy)


def draw_couple(key, part):
    base = 0.7 * jax.random.normal(jax.random.fold_in(key, 31), (K, N, N), jnp.float32) / math.sqrt(2.0 * N)
    return base + jnp.swapaxes(base, 1, 2)


def level_of(stream_key, extent, cuts, smallest, top_value):
    gain, own = 1.0, jax.random.fold_in(stream_key, 6)
    for dim, shards_of in cuts:
        draws = jnp.exp(jax.random.uniform(jax.random.fold_in(own, dim), (shards_of,), jnp.float32, smallest / len(cuts), top_value / len(cuts)))
        gain = gain * jnp.repeat(draws, extent[dim] // shards_of).reshape([-1 if axis == dim else 1 for axis in range(len(extent))])
    return gain


def scatter_about(key, shape, width, bound, cuts=(), held_as=jnp.bfloat16):
    array = jax.random.normal(key, shape, jnp.float32) * width
    if len(cuts) > 0:
        array = level_of(key, shape, cuts, -0.22, 0.18) * array
    return jnp.clip(array, min=-bound, max=bound).astype(held_as)


def setup_inputs(seed: int = 0) -> dict:
    key_list = jax.random.split(jax.random.key(seed), 14)
    return {
        "shallow_state": scatter_about(key_list[0], (SH_TOTAL, 2, N, N), 1.0, 6.0, ((0, 8),), jnp.float32),
        "shallow_prev": scatter_about(key_list[1], (SH_TOTAL, 2, N, N), 1.0, 6.0, ((0, 8),), jnp.float32),
        "deep_state": scatter_about(key_list[2], (DEEP_TOTAL, 2, N, N), 1.0, 6.0, ((0, 32),), jnp.float32),
        "deep_prev": scatter_about(key_list[3], (DEEP_TOTAL, 2, N, N), 1.0, 6.0, ((0, 32),), jnp.float32),
        "hamilton": draw_hamilton(jax.random.fold_in(key_list[13], 71), 0),
        "couple": draw_couple(jax.random.fold_in(key_list[13], 71), 0),
        "gamma": jnp.clip(jnp.exp(jax.random.uniform(key_list[6], (K,), jnp.float32, math.log(0.2), math.log(5.0))), 0.2, 5.0),
        "coef_real": jnp.clip(jnp.exp(jax.random.uniform(key_list[7], (K,), jnp.float32, math.log(0.2), math.log(2.0))), 0.2, 2.0),
        "coef_imag": jnp.clip(jnp.exp(jax.random.uniform(key_list[8], (K,), jnp.float32, math.log(0.1), math.log(1.0))), 0.1, 1.0),
        "shallow_bath": draw_shallow_bath(jax.random.fold_in(key_list[13], 71), 0),
        "shallow_lower": draw_shallow_lower(jax.random.fold_in(key_list[13], 71), 0),
        "deep_bath": draw_deep_bath(jax.random.fold_in(key_list[13], 71), 0),
        "deep_lower": draw_deep_lower(jax.random.fold_in(key_list[13], 71), 0),
    }


half_step = 0.1


def pick_rates(baths, rates):
    matches = (baths[:, None] == jnp.arange(rates.shape[0], dtype=jnp.int32)[None, :]).astype(jnp.float32)
    return jnp.dot(matches, rates, precision=lax.Precision.HIGHEST)


def with_operator(operator, matrices):
    before = jnp.einsum("unm,umj->unj", operator, matrices, precision=lax.Precision.HIGHEST)
    after = jnp.einsum("unm,umj->unj", matrices, operator, precision=lax.Precision.HIGHEST)
    return before - after, before + after


def with_hamilton(hamilton, matrices):
    before = jnp.einsum("nm,umj->unj", hamilton, matrices, precision=lax.Precision.HIGHEST)
    after = jnp.einsum("unm,mj->unj", matrices, hamilton, precision=lax.Precision.HIGHEST)
    return before - after


def own_terms(trial, baths, hamilton, gamma):
    damping = jnp.zeros((trial.shape[0],), jnp.float32)
    for column in range(baths.shape[1]):
        damping = damping + pick_rates(baths[:, column], gamma)
    real_part = with_hamilton(hamilton, trial[:, 1]) - damping[:, None, None] * trial[:, 0]
    imag_part = -with_hamilton(hamilton, trial[:, 0]) - damping[:, None, None] * trial[:, 1]
    return jnp.stack([real_part, imag_part], 1)


def lower_terms(baths, lowers, source, couple, coef_real, coef_imag):
    result = jnp.zeros((baths.shape[0],) + source.shape[1:], jnp.float32)
    for column in range(baths.shape[1]):
        usable = ((baths[:, column] >= 0) & (lowers[:, column] >= 0)).astype(jnp.float32)
        neighbour = source[jnp.maximum(lowers[:, column], 0)]
        operator = couple[jnp.maximum(baths[:, column], 0)]
        comm_real, anti_real = with_operator(operator, neighbour[:, 0])
        comm_imag, anti_imag = with_operator(operator, neighbour[:, 1])
        scale_a = (pick_rates(baths[:, column], coef_real) * usable)[:, None, None]
        scale_b = (pick_rates(baths[:, column], coef_imag) * usable)[:, None, None]
        real_part = scale_a * comm_imag - scale_b * anti_real
        imag_part = -scale_a * comm_real - scale_b * anti_imag
        result = result + jnp.stack([real_part, imag_part], 1)
    return result


def pushed_terms(baths, lowers, trial, couple, dump_row):
    pieces = []
    targets = []
    for column in range(baths.shape[1]):
        leading = (baths[:, column] >= 0) & (lowers[:, column] >= 0)
        if column > 0:
            leading = leading & (baths[:, column] != baths[:, column - 1])
        operator = couple[jnp.maximum(baths[:, column], 0)]
        comm_real, unused_real = with_operator(operator, trial[:, 0])
        comm_imag, unused_imag = with_operator(operator, trial[:, 1])
        pieces.append(jnp.stack([comm_imag, -comm_real], 1))
        targets.append(jnp.where(leading, lowers[:, column], dump_row).astype(jnp.int32))
    return pieces, targets


def reference(shallow_state, shallow_prev, deep_state, deep_prev, hamilton, couple, gamma, coef_real, coef_imag, shallow_bath, shallow_lower, deep_bath, deep_lower):
    shallow_trial = shallow_state + half_step * shallow_prev
    deep_trial = deep_state + half_step * deep_prev
    row_count = shallow_trial.shape[0]
    deep_slope = own_terms(deep_trial, deep_bath, hamilton, gamma) + lower_terms(deep_bath, deep_lower, shallow_trial, couple, coef_real, coef_imag)
    shallow_slope = own_terms(shallow_trial, shallow_bath, hamilton, gamma) + lower_terms(shallow_bath, shallow_lower, shallow_trial, couple, coef_real, coef_imag)
    deep_pieces, deep_targets = pushed_terms(deep_bath, deep_lower, deep_trial, couple, row_count)
    top_pieces, top_targets = pushed_terms(shallow_bath, shallow_lower, shallow_trial, couple, row_count)
    upper = jax.ops.segment_sum(jnp.concatenate(deep_pieces + top_pieces, 0), jnp.concatenate(deep_targets + top_targets, 0), num_segments=row_count + 1)[:row_count]
    return shallow_slope + upper, deep_slope
```

```python
import jax
import jax.numpy as jnp
from jax import lax
from jax.experimental import pallas as pl
from jax.experimental.pallas import tpu as pltpu
from jax.sharding import PartitionSpec as P

half_step = 0.1


def split(x):
    high = x.astype(jnp.bfloat16)
    low = (x - high.astype(jnp.float32)).astype(jnp.bfloat16)
    return high, low


def operator_tiles(operators):
    rounded = lax.reduce_precision(operators, 8, 7)
    high = rounded.astype(jnp.bfloat16)
    low = (operators - rounded).astype(jnp.bfloat16)
    zero = jnp.zeros_like(high)
    left = jnp.concatenate(
        [jnp.concatenate([high, high], 2), jnp.concatenate([low, zero], 2)], 1
    )
    right = jnp.concatenate(
        [jnp.concatenate([high, low], 2), jnp.concatenate([high, zero], 2)], 1
    )
    return left, right


def matrix_tiles(x):
    n = x.shape[1]
    high, low = split(x)
    beside = jnp.concatenate(
        [jnp.concatenate([high[0], high[1]], 1), jnp.concatenate([low[0], low[1]], 1)], 0
    )
    below = jnp.concatenate([high.reshape(2 * n, n), low.reshape(2 * n, n)], 1)
    return beside, below


def products(left, right, beside, below):
    n = beside.shape[0] // 2
    a = jnp.dot(left, beside, preferred_element_type=jnp.float32)
    b = jnp.dot(below, right, preferred_element_type=jnp.float32)
    a = a[:n] + a[n:]
    b = b[:, :n] + b[:, n:]
    return a[:, :n], a[:, n:], b[:n], b[n:]


def pack(source, target, bath, coef, keep):
    word = source + (target << 10) + (bath << 20) + (coef << 25)
    return jnp.where(keep, word, -1)


def unpack(word):
    return word & 1023, (word >> 10) & 1023, (word >> 20) & 31, word >> 25


def list_live(words, live, idle):
    def add(index, found):
        @pl.when(words[index] >= 0)
        def _():
            live[found] = words[index]

        return found + (words[index] >= 0).astype(jnp.int32)

    found = lax.fori_loop(0, words.shape[0], add, 0)
    for extra in range(width):
        live[found + extra] = idle << 10
    return found


def run(copies):
    for copy in copies:
        copy.start()
    for copy in copies:
        copy.wait()


width = 2
vmem_bytes = 60 * 1024 * 1024


def push_kernel(first, own, *refs):
    words, damping = refs[:2]
    x_ref, left_tiles, right_tiles = refs[2:5]
    refs = refs[5:]
    if not first:
        before, refs = refs[:2], refs[2:]
    if own:
        own_ref, refs = refs[0], refs[1:]
    after, refs = refs[:2], refs[2:]
    total, left_ref, right_ref, beside_ref, below_ref, live, sems = refs
    count = x_ref.shape[0]
    half = (total.shape[0] - 1) // 2
    fetch = [
        pltpu.make_async_copy(left_tiles, left_ref, sems.at[2]),
        pltpu.make_async_copy(right_tiles, right_ref, sems.at[3]),
    ]
    for copy in fetch:
        copy.start()
    loads = []
    if first:
        total[...] = jnp.zeros_like(total)
    else:
        loads = [
            pltpu.make_async_copy(before[h], total.at[pl.ds(h * half, half)], sems.at[h])
            for h in range(2)
        ]
        for copy in loads:
            copy.start()
    found = list_live(words, live, 2 * half)

    @pl.loop(0, count)
    def _(slot):
        beside, below = matrix_tiles(x_ref[slot])
        beside_ref[slot] = beside
        below_ref[slot] = below

    for copy in fetch:
        copy.wait()
    if own:
        last = left_ref.shape[0] - 1
        group = width if count % width == 0 else 1

        @pl.loop(0, count // group)
        def _(step):
            slots = [step * group + extra for extra in range(group)]
            made = [
                products(left_ref[last], right_ref[last], beside_ref[slot], below_ref[slot])
                for slot in slots
            ]
            for slot, (lr, li, rr, ri) in zip(slots, made):
                rate = damping[slot]
                own_ref[slot, 0] = (li - ri) - rate * x_ref[slot, 0]
                own_ref[slot, 1] = (rr - lr) - rate * x_ref[slot, 1]

    for copy in loads:
        copy.wait()

    @pl.loop(0, (found + width - 1) // width)
    def _(step):
        made = []
        for extra in range(width):
            slot, row, bath, _ = unpack(live[step * width + extra])
            made.append(
                (row, products(left_ref[bath], right_ref[bath], beside_ref[slot], below_ref[slot]))
            )
        for row, (lr, li, rr, ri) in made:
            total[row, 0] += li - ri
            total[row, 1] += rr - lr

    run(
        [
            pltpu.make_async_copy(total.at[pl.ds(h * half, half)], after[h], sems.at[h])
            for h in range(2)
        ]
    )


def push(x, words, damping, tiles, row_count, before=None, own=False):
    count, _, n, _ = x.shape
    smem = pl.BlockSpec(memory_space=pltpu.SMEM)
    vmem = pl.BlockSpec(memory_space=pltpu.VMEM)
    anywhere = pl.BlockSpec(memory_space=pl.ANY)
    half = jax.ShapeDtypeStruct((row_count // 2, 2, n, n), jnp.float32)
    first = before is None
    extra = () if first else tuple(before)
    return pl.pallas_call(
        lambda *refs: push_kernel(first, own, *refs),
        in_specs=[smem] * 2 + [vmem] + [anywhere] * (2 + len(extra)),
        out_specs=([vmem] if own else []) + [anywhere] * 2,
        scratch_shapes=[
            pltpu.VMEM((row_count + 1, 2, n, n), jnp.float32),
            pltpu.VMEM(tiles[0].shape, jnp.bfloat16),
            pltpu.VMEM(tiles[1].shape, jnp.bfloat16),
            pltpu.VMEM((count, 2 * n, 2 * n), jnp.bfloat16),
            pltpu.VMEM((count, 2 * n, 2 * n), jnp.bfloat16),
            pltpu.SMEM((words.shape[0] + width,), jnp.int32),
            pltpu.SemaphoreType.DMA((4,)),
        ],
        out_shape=([jax.ShapeDtypeStruct(x.shape, jnp.float32)] if own else []) + [half] * 2,
        compiler_params=pltpu.CompilerParams(vmem_limit_bytes=vmem_bytes),
        cost_estimate=pl.CostEstimate(
            flops=count * 4 * 16 * n**3, bytes_accessed=count * 8 * n * n, transcendentals=0
        ),
    )(words, damping, x, tiles[0], tiles[1], *extra)


def pull_kernel(parts, *refs):
    words, commute, anti, left_tiles, right_tiles = refs[:5]
    sources = refs[5 : 5 + parts]
    out_ref, held, total, left_ref, right_ref, live, sems = refs[5 + parts :]
    size = held.shape[0] // parts
    count = total.shape[0] - 1
    loads = [
        pltpu.make_async_copy(left_tiles, left_ref, sems.at[parts]),
        pltpu.make_async_copy(right_tiles, right_ref, sems.at[parts + 1]),
    ] + [
        pltpu.make_async_copy(sources[p], held.at[pl.ds(p * size, size)], sems.at[p])
        for p in range(parts)
    ]
    for copy in loads:
        copy.start()
    found = list_live(words, live, count)
    total[...] = jnp.zeros_like(total)
    for copy in loads:
        copy.wait()

    @pl.loop(0, (found + width - 1) // width)
    def _(step):
        made = []
        for extra in range(width):
            source, target, bath, coef = unpack(live[step * width + extra])
            tiled = matrix_tiles(held[source])
            made.append((target, coef, products(left_ref[bath], right_ref[bath], *tiled)))
        for target, coef, (lr, li, rr, ri) in made:
            a = commute[coef]
            b = anti[coef]
            total[target, 0] += a * (li - ri) - b * (lr + rr)
            total[target, 1] += a * (rr - lr) - b * (li + ri)

    run([pltpu.make_async_copy(total.at[pl.ds(0, count)], out_ref, sems.at[0])])


def pull(count, words, coefs, tiles, sources):
    size, _, n, _ = sources[0].shape
    parts = len(sources)
    smem = pl.BlockSpec(memory_space=pltpu.SMEM)
    anywhere = pl.BlockSpec(memory_space=pl.ANY)
    return pl.pallas_call(
        lambda *refs: pull_kernel(parts, *refs),
        in_specs=[smem] * 3 + [anywhere] * (2 + parts),
        out_specs=anywhere,
        scratch_shapes=[
            pltpu.VMEM((parts * size, 2, n, n), jnp.float32),
            pltpu.VMEM((count + 1, 2, n, n), jnp.float32),
            pltpu.VMEM(tiles[0].shape, jnp.bfloat16),
            pltpu.VMEM(tiles[1].shape, jnp.bfloat16),
            pltpu.SMEM((words.shape[0] + width,), jnp.int32),
            pltpu.SemaphoreType.DMA((parts + 2,)),
        ],
        out_shape=jax.ShapeDtypeStruct((count, 2, n, n), jnp.float32),
        compiler_params=pltpu.CompilerParams(vmem_limit_bytes=vmem_bytes),
        cost_estimate=pl.CostEstimate(
            flops=count * 3 * 16 * n**3, bytes_accessed=parts * size * 8 * n * n, transcendentals=0
        ),
    )(words, *coefs, tiles[0], tiles[1], *sources)


def pick_rates(baths, rates):
    matches = baths[..., None] == jnp.arange(rates.shape[0], dtype=jnp.int32)
    return jnp.sum(jnp.where(matches, rates, 0.0), -1)


def line_stages(count, place):
    middle = count // 2
    added = lambda x, got: x + got

    def send(pairs):
        return lambda x: lax.ppermute(x, "row", pairs)

    stages = []
    for hop in range(middle - 1):
        stages.append((send([(hop, hop + 1), (count - 1 - hop, count - 2 - hop)]), added))
    stages.append((send([(middle - 1, middle), (middle, middle - 1)]), added))
    for hop in range(middle - 1, 0, -1):
        there = (place == hop - 1) | (place == count - hop)
        stages.append(
            (
                send([(hop, hop - 1), (count - 1 - hop, count - hop)]),
                lambda x, got, there=there: jnp.where(there, got, x),
            )
        )
    return stages


def together(*arrays):
    return lax.optimization_barrier(arrays)


def body(
    shallow_state,
    shallow_prev,
    deep_state,
    deep_prev,
    hamilton,
    couple,
    gamma,
    coef_real,
    coef_imag,
    shallow_bath,
    shallow_lower,
    deep_bath,
    deep_lower,
):
    row_count = lax.axis_size("row")
    col_count = lax.axis_size("col")
    slot_count = shallow_state.shape[0]
    deep_count = deep_state.shape[0]
    per_row = slot_count // row_count
    side_size = col_count // 2
    bits = side_size.bit_length() - 1
    row = lax.axis_index("row")
    col = lax.axis_index("col")
    side = col // side_size
    place = col % side_size

    def swap(x, distance):
        return lax.ppermute(x, "col", [(i, i ^ distance) for i in range(col_count)])

    bath_count = couple.shape[0]
    first_row = row * per_row

    def part_of(x):
        return lax.dynamic_slice_in_dim(x, first_row, per_row, 0)

    def columns(top, deep):
        return [x[:, unit] for x in (top, deep) for unit in range(x.shape[1])]

    table = jnp.concatenate(
        columns(shallow_bath, deep_bath) + columns(shallow_lower, deep_lower), 0
    )
    peers = [side_size] + list(range(1, side_size))
    tables = [table] + [swap(table, distance) for distance in peers]
    deep_trial = deep_state + half_step * deep_prev
    shallow_trial = shallow_state + half_step * shallow_prev
    *tables, deep_trial, shallow_trial = together(*tables, deep_trial, shallow_trial)
    theirs = swap(deep_trial, side_size)
    held = {0: shallow_trial}

    tables = jnp.stack(tables, 0)
    wide = table.shape[0] // 2
    top_wide = 2 * slot_count
    baths, lowers = tables[:, :wide], tables[:, wide:]
    none = jnp.full_like(baths, -1)
    previous = jnp.concatenate(
        [
            none[:, :slot_count],
            baths[:, :slot_count],
            none[:, :deep_count],
            baths[:, top_wide : wide - deep_count],
        ],
        1,
    )
    numbers = jnp.arange(wide, dtype=jnp.int32)[None, :]
    slots = jnp.where(
        numbers < top_wide, numbers % slot_count, (numbers - top_wide) % deep_count
    )
    there = (baths >= 0) & (lowers >= 0)
    leading = there & (baths != previous)
    baths = jnp.maximum(baths, 0)
    owner = jnp.maximum(lowers, 0) // slot_count
    offset = jnp.maximum(lowers, 0) % slot_count
    near = owner // side_size == side
    relative = (owner % side_size) ^ place
    mirrored = jnp.zeros_like(relative)
    for bit in range(bits):
        mirrored = mirrored | (((relative >> bit) & 1) << (bits - 1 - bit))
    push_words = pack(slots, mirrored * slot_count + offset, baths, 0, leading & near)
    source = relative * slot_count + offset
    pull_words = pack(source, slots, baths, baths, there & near)
    half_number = jnp.arange(tables.shape[0], dtype=jnp.int32)[:, None]
    part_words = pack(
        source,
        slots % per_row + half_number * per_row,
        baths,
        baths,
        there & near & (slots // per_row == row),
    )[:2, :top_wide]
    key = jnp.maximum(half_number - 1, 0)
    to_mine = owner == col
    to_other = owner == (col ^ side_size)
    raise_words = pack(
        key * slot_count + slots,
        offset % per_row + jnp.where(to_mine, 0, per_row),
        baths,
        bath_count,
        leading & (to_mine | to_other) & (offset // per_row == row),
    )[:, :top_wide]
    places = jnp.arange(per_row, dtype=jnp.int32)
    own_words = pack(first_row + places, places, bath_count, bath_count, places >= 0)
    part_words = jnp.concatenate(
        [own_words, part_words[0], part_words[1], raise_words[0]]
        + [raise_words[1 + distance] for distance in range(1, side_size)],
        0,
    )
    push_mine, push_other = push_words[0, top_wide:], push_words[1, top_wide:]
    pull_mine, pull_other = pull_words[0, top_wide:], pull_words[1, top_wide:]
    coefs = [
        jnp.concatenate([coef_real, jnp.ones((1,), jnp.float32)], 0),
        jnp.concatenate([coef_imag, jnp.zeros((1,), jnp.float32)], 0),
    ]

    tiles = operator_tiles(jnp.concatenate([couple, hamilton[None]], 0))
    total_rows = side_size * slot_count
    damping = jnp.sum(pick_rates(deep_bath, gamma), 1)
    part_damping = jnp.sum(pick_rates(part_of(shallow_bath), gamma), 1)[:, None, None, None]
    part_own = part_damping * part_of(shallow_trial)
    push_mine, push_other, pull_mine, pull_other, part_words = together(
        push_mine, push_other, pull_mine, pull_other, part_words
    )
    own, keep, send = push(deep_trial, push_mine, damping, tiles, total_rows, own=True)
    for bit in range(bits - 1, -1, -1):
        for place_key in list(held):
            held[place_key | (1 << bit)] = swap(held[place_key], 1 << bit)
            if place_key == 0 and bit == bits - 1:
                held[1 << bit], own = together(held[1 << bit], own)
    sources = [held[k] for k in range(side_size)]
    keep, send = push(theirs, push_other, damping, tiles, total_rows, (keep, send))
    part_words, send = together(part_words, send)
    got = swap(send, 1)
    parts = pull(2 * per_row, part_words, coefs, tiles, sources)
    got, parts = together(got, parts)
    part = parts[:per_row] - part_own + swap(parts[per_row:], side_size)

    def piece(x, block, index):
        start = block * slot_count + index * per_row
        return x[start : start + per_row]

    def blocks_of(index, low, high):
        return [piece(keep, b, index) + piece(got, b, index) for b in range(low, high)]

    middle = side_size // 4
    stages = line_stages(row_count, row)
    value, coming, fold = {}, {}, {}
    sent = blocks_of(0, middle, 2 * middle)
    pull_other, *sent = together(pull_other, *sent)
    fresh = [swap(x, 2) for x in sent]
    away = pull(deep_count, pull_other, coefs, tiles, sources)
    for tick in range(row_count + len(stages)):
        active = list(coming)
        came = [coming[k] for k in active]
        passing = [keep, got, pull_mine]
        if tick == 0:
            passing.append(away)
        if tick == 1:
            passing.append(deep_slope)
        everything = together(*came, *fresh, *passing)
        came = everything[: len(came)]
        fresh = everything[len(came) : len(came) + len(fresh)]
        passing = everything[len(came) + len(fresh) :]
        keep, got, pull_mine = passing[:3]
        if tick == 1:
            deep_slope = passing[3]
        coming = {}
        for k, moved in zip(active, came):
            value[k] = fold[k](value[k], moved)
        if tick < row_count:
            blocks = [a + b for a, b in zip(blocks_of(tick, 0, middle), fresh)]
            for bit in range(2, bits):
                size = len(blocks) // 2
                blocks = [blocks[b] + swap(blocks[size + b], 1 << bit) for b in range(size)]
            value[tick] = blocks[0] + jnp.where(row == tick, part, 0.0)
        fresh = []
        if tick + 1 < row_count:
            fresh = [swap(x, 2) for x in blocks_of(tick + 1, middle, 2 * middle)]
        for k in value:
            if 0 <= tick - k < len(stages):
                move, fold[k] = stages[tick - k]
                coming[k] = move(value[k])
        if tick == 0:
            away = swap(passing[3], side_size)
            deep_slope = own + pull(deep_count, pull_mine, coefs, tiles, sources)
    for k, moved in coming.items():
        value[k] = fold[k](value[k], moved)
    chunks = [value[k] for k in range(row_count)]
    deep_slope = deep_slope + away
    shallow_slope = jnp.concatenate(chunks, 0)
    return (shallow_slope, deep_slope)


def solution(mesh):
    placed = (
        P("col", None, None, None),
        P("col", None, None, None),
        P(("row", "col"), None, None, None),
        P(("row", "col"), None, None, None),
        P(),
        P(),
        P(),
        P(),
        P(),
        P("col", None),
        P("col", None),
        P(("row", "col"), None),
        P(("row", "col"), None),
    )
    return jax.shard_map(
        body,
        mesh=mesh,
        in_specs=placed,
        out_specs=(P("col", None, None, None), P(("row", "col"), None, None, None)),
        check_vma=False,
    )
```

```python
import jax
import jax.numpy as jnp
from jax import lax
from jax.experimental import pallas as pl
from jax.experimental.pallas import tpu as pltpu
from jax.sharding import PartitionSpec as P


half_step = 0.1


def split(x):
    high = x.astype(jnp.bfloat16)
    low = (x - high.astype(jnp.float32)).astype(jnp.bfloat16)
    return high, low


def operator_tiles(operators):
    rounded = lax.reduce_precision(operators, 8, 7)
    high = rounded.astype(jnp.bfloat16)
    low = (operators - rounded).astype(jnp.bfloat16)
    zero = jnp.zeros_like(high)
    left = jnp.concatenate(
        [jnp.concatenate([high, high], 2), jnp.concatenate([low, zero], 2)], 1
    )
    right = jnp.concatenate(
        [jnp.concatenate([high, low], 2), jnp.concatenate([high, zero], 2)], 1
    )
    return left, right


def matrix_tiles(x):
    n = x.shape[1]
    high, low = split(x)
    beside = jnp.concatenate(
        [jnp.concatenate([high[0], high[1]], 1), jnp.concatenate([low[0], low[1]], 1)], 0
    )
    below = jnp.concatenate([high.reshape(2 * n, n), low.reshape(2 * n, n)], 1)
    return beside, below


def products(left, right, beside, below):
    n = beside.shape[0] // 2
    a = jnp.dot(left, beside, preferred_element_type=jnp.float32)
    b = jnp.dot(below, right, preferred_element_type=jnp.float32)
    a = a[:n] + a[n:]
    b = b[:, :n] + b[:, n:]
    return a[:, :n], a[:, n:], b[:n], b[n:]


def pack(source, target, bath, coef, keep):
    word = source + (target << 10) + (bath << 20) + (coef << 25)
    return jnp.where(keep, word, -1)


def unpack(word):
    return word & 1023, (word >> 10) & 1023, (word >> 20) & 31, word >> 25


def list_live(words, live, idle):
    def add(index, found):
        @pl.when(words[index] >= 0)
        def _():
            live[found] = words[index]

        return found + (words[index] >= 0).astype(jnp.int32)

    found = lax.fori_loop(0, words.shape[0], add, 0)
    for extra in range(width):
        live[found + extra] = idle << 10
    return found


def run(copies):
    for copy in copies:
        copy.start()
    for copy in copies:
        copy.wait()


width = 2
finer = 1
vmem_bytes = 60 * 1024 * 1024


def push_kernel(own, *refs):
    words, damping = refs[:2]
    x_ref, left_tiles, right_tiles = refs[2:5]
    refs = refs[5:]
    if own:
        own_ref, refs = refs[0], refs[1:]
    after, refs = refs[:2], refs[2:]
    total, left_ref, right_ref, beside_ref, below_ref, live, sems = refs
    count = x_ref.shape[0]
    half = (total.shape[0] - 1) // 2
    fetch = [
        pltpu.make_async_copy(left_tiles, left_ref, sems.at[2]),
        pltpu.make_async_copy(right_tiles, right_ref, sems.at[3]),
    ]
    for copy in fetch:
        copy.start()
    total[...] = jnp.zeros_like(total)
    found = list_live(words, live, 2 * half)

    @pl.loop(0, count)
    def _(slot):
        beside, below = matrix_tiles(x_ref[slot])
        beside_ref[slot] = beside
        below_ref[slot] = below

    for copy in fetch:
        copy.wait()
    if own:
        last = left_ref.shape[0] - 1
        group = width if count % width == 0 else 1

        @pl.loop(0, count // group)
        def _(step):
            slots = [step * group + extra for extra in range(group)]
            made = [
                products(left_ref[last], right_ref[last], beside_ref[slot], below_ref[slot])
                for slot in slots
            ]
            for slot, (lr, li, rr, ri) in zip(slots, made):
                rate = damping[slot]
                own_ref[slot, 0] = (li - ri) - rate * x_ref[slot, 0]
                own_ref[slot, 1] = (rr - lr) - rate * x_ref[slot, 1]

    @pl.loop(0, (found + width - 1) // width)
    def _(step):
        made = []
        for extra in range(width):
            slot, row, bath, _ = unpack(live[step * width + extra])
            made.append(
                (row, products(left_ref[bath], right_ref[bath], beside_ref[slot], below_ref[slot]))
            )
        for row, (lr, li, rr, ri) in made:
            total[row, 0] += li - ri
            total[row, 1] += rr - lr

    run(
        [
            pltpu.make_async_copy(total.at[pl.ds(h * half, half)], after[h], sems.at[h])
            for h in range(2)
        ]
    )


def push(x, words, damping, tiles, row_count, own=False):
    count, _, n, _ = x.shape
    smem = pl.BlockSpec(memory_space=pltpu.SMEM)
    vmem = pl.BlockSpec(memory_space=pltpu.VMEM)
    anywhere = pl.BlockSpec(memory_space=pl.ANY)
    half = jax.ShapeDtypeStruct((row_count // 2, 2, n, n), jnp.float32)
    return pl.pallas_call(
        lambda *refs: push_kernel(own, *refs),
        in_specs=[smem] * 2 + [vmem] + [anywhere] * 2,
        out_specs=([vmem] if own else []) + [anywhere] * 2,
        scratch_shapes=[
            pltpu.VMEM((row_count + 1, 2, n, n), jnp.float32),
            pltpu.VMEM(tiles[0].shape, jnp.bfloat16),
            pltpu.VMEM(tiles[1].shape, jnp.bfloat16),
            pltpu.VMEM((count, 2 * n, 2 * n), jnp.bfloat16),
            pltpu.VMEM((count, 2 * n, 2 * n), jnp.bfloat16),
            pltpu.SMEM((words.shape[0] + width,), jnp.int32),
            pltpu.SemaphoreType.DMA((4,)),
        ],
        out_shape=([jax.ShapeDtypeStruct(x.shape, jnp.float32)] if own else []) + [half] * 2,
        compiler_params=pltpu.CompilerParams(vmem_limit_bytes=vmem_bytes),
        cost_estimate=pl.CostEstimate(
            flops=count * 4 * 16 * n**3, bytes_accessed=count * 8 * n * n, transcendentals=0
        ),
    )(words, damping, x, tiles[0], tiles[1])


def pull_kernel(parts, begin, *refs):
    words, commute, anti, left_tiles, right_tiles = refs[:5]
    sources = refs[5 : 5 + parts]
    refs = refs[5 + parts :]
    if begin is not None:
        base, refs = refs[0], refs[1:]
    out_ref, held, total, left_ref, right_ref, live, sems = refs
    size = held.shape[0] // parts
    count = total.shape[0] - 1
    loads = [
        pltpu.make_async_copy(left_tiles, left_ref, sems.at[parts]),
        pltpu.make_async_copy(right_tiles, right_ref, sems.at[parts + 1]),
    ] + [
        pltpu.make_async_copy(sources[p], held.at[pl.ds(p * size, size)], sems.at[p])
        for p in range(parts)
    ]
    if begin is not None:
        before = base.at[pl.ds(begin, count)]
        loads.append(pltpu.make_async_copy(before, total.at[pl.ds(0, count)], sems.at[parts + 2]))
    for copy in loads:
        copy.start()
    found = list_live(words, live, count)
    if begin is None:
        total[...] = jnp.zeros_like(total)
    for copy in loads:
        copy.wait()

    @pl.loop(0, (found + width - 1) // width)
    def _(step):
        made = []
        for extra in range(width):
            source, target, bath, coef = unpack(live[step * width + extra])
            tiled = matrix_tiles(held[source])
            made.append((target, coef, products(left_ref[bath], right_ref[bath], *tiled)))
        for target, coef, (lr, li, rr, ri) in made:
            a = commute[coef]
            b = anti[coef]
            total[target, 0] += a * (li - ri) - b * (lr + rr)
            total[target, 1] += a * (rr - lr) - b * (li + ri)

    run([pltpu.make_async_copy(total.at[pl.ds(0, count)], out_ref, sems.at[0])])


def pull(count, words, coefs, tiles, sources, base=None, begin=None):
    size, _, n, _ = sources[0].shape
    parts = len(sources)
    extra = () if base is None else (base,)
    smem = pl.BlockSpec(memory_space=pltpu.SMEM)
    anywhere = pl.BlockSpec(memory_space=pl.ANY)
    return pl.pallas_call(
        lambda *refs: pull_kernel(parts, begin, *refs),
        in_specs=[smem] * 3 + [anywhere] * (2 + parts + len(extra)),
        out_specs=anywhere,
        scratch_shapes=[
            pltpu.VMEM((parts * size, 2, n, n), jnp.float32),
            pltpu.VMEM((count + 1, 2, n, n), jnp.float32),
            pltpu.VMEM(tiles[0].shape, jnp.bfloat16),
            pltpu.VMEM(tiles[1].shape, jnp.bfloat16),
            pltpu.SMEM((words.shape[0] + width,), jnp.int32),
            pltpu.SemaphoreType.DMA((parts + 3,)),
        ],
        out_shape=jax.ShapeDtypeStruct((count, 2, n, n), jnp.float32),
        compiler_params=pltpu.CompilerParams(vmem_limit_bytes=vmem_bytes),
        cost_estimate=pl.CostEstimate(
            flops=count * 3 * 16 * n**3, bytes_accessed=parts * size * 8 * n * n, transcendentals=0
        ),
    )(words, *coefs, tiles[0], tiles[1], *sources, *extra)


def pick_rates(baths, rates):
    matches = baths[..., None] == jnp.arange(rates.shape[0], dtype=jnp.int32)
    return jnp.sum(jnp.where(matches, rates, 0.0), -1)


def line_stages(count, place):
    middle = count // 2
    added = lambda x, got: x + got

    def send(pairs):
        return lambda x: lax.ppermute(x, "row", pairs)

    stages = []
    for hop in range(middle - 1):
        stages.append((send([(hop, hop + 1), (count - 1 - hop, count - 2 - hop)]), added))
    stages.append((send([(middle - 1, middle), (middle, middle - 1)]), added))
    for hop in range(middle - 1, 0, -1):
        there = (place == hop - 1) | (place == count - hop)
        stages.append(
            (
                send([(hop, hop - 1), (count - 1 - hop, count - hop)]),
                lambda x, got, there=there: jnp.where(there, got, x),
            )
        )
    return stages


def together(*arrays):
    return lax.optimization_barrier(arrays)


def section(
    shallow_state,
    shallow_prev,
    deep_state,
    deep_prev,
    hamilton,
    couple,
    gamma,
    coef_real,
    coef_imag,
    shallow_bath,
    shallow_lower,
    deep_bath,
    deep_lower,
):
    row_count = lax.axis_size("row")
    col_count = lax.axis_size("col")
    slot_count = shallow_state.shape[0]
    deep_count = deep_state.shape[0]
    per_row = slot_count // row_count
    side_size = col_count // 2
    bits = side_size.bit_length() - 1
    row = lax.axis_index("row")
    col = lax.axis_index("col")
    side = col // side_size
    place = col % side_size

    def swap(x, distance):
        return lax.ppermute(x, "col", [(i, i ^ distance) for i in range(col_count)])

    bath_count = couple.shape[0]
    first_row = row * per_row

    def part_of(x):
        return lax.dynamic_slice_in_dim(x, first_row, per_row, 0)

    def columns(top, deep):
        return [x[:, unit] for x in (top, deep) for unit in range(x.shape[1])]

    table = jnp.concatenate(
        columns(shallow_bath, deep_bath) + columns(shallow_lower, deep_lower), 0
    )
    deep_trial = deep_state + half_step * deep_prev
    other_table = swap(table, side_size)
    theirs = swap(deep_trial, side_size)
    shallow_trial = shallow_state + half_step * shallow_prev
    held = {0: shallow_trial}
    for bit in range(bits - 1, -1, -1):
        for place_key in list(held):
            held[place_key | (1 << bit)] = swap(held[place_key], 1 << bit)
    places = jnp.arange(per_row, dtype=jnp.int32)
    wide = table.shape[0] // 2
    top_wide = 2 * slot_count
    numbers = jnp.arange(wide, dtype=jnp.int32)
    slots = jnp.where(
        numbers < top_wide, numbers % slot_count, (numbers - top_wide) % deep_count
    )
    in_plane = slots // per_row == row
    half = side_size // 2 * slot_count

    def read(table):
        baths, lowers = table[:wide], table[wide:]
        none = jnp.full_like(baths, -1)
        previous = jnp.concatenate(
            [
                none[:slot_count],
                baths[:slot_count],
                none[:deep_count],
                baths[top_wide : wide - deep_count],
            ],
            0,
        )
        there = (baths >= 0) & (lowers >= 0)
        owner = jnp.maximum(lowers, 0) // slot_count
        offset = jnp.maximum(lowers, 0) % slot_count
        return jnp.maximum(baths, 0), there, there & (baths != previous), owner, offset

    def words_of(table, number):
        baths, there, leading, owner, offset = read(table)
        near = owner // side_size == side
        relative = (owner % side_size) ^ place
        mirrored = jnp.zeros_like(relative)
        for bit in range(bits):
            mirrored = mirrored | (((relative >> bit) & 1) << (bits - 1 - bit))
        source = relative * slot_count + offset
        pushed = pack(slots, mirrored * slot_count + offset, baths, 0, leading & near)
        early = there & near & (source < half)
        early = pack(source, slots + number * deep_count, baths, baths, early)
        late = pack(source - half, slots, baths, baths, there & near & (source >= half))
        rows = slots % per_row + number * per_row
        part = pack(source, rows, baths, baths, there & near & in_plane)
        return pushed[top_wide:], early[top_wide:], late[top_wide:], part[:top_wide]

    def raised_of(table, key):
        baths, _, leading, owner, offset = read(table)
        to_mine = owner == col
        to_other = owner == (col ^ side_size)
        live = leading & (to_mine | to_other) & (offset // per_row == row)
        rows = offset % per_row + jnp.where(to_mine, 0, per_row)
        return pack(key * slot_count + slots, rows, baths, bath_count, live)[:top_wide]

    push_mine, early_mine, late_mine, part_mine = words_of(table, 0)
    push_other, early_other, late_other, part_other = words_of(other_table, 1)
    early_words = jnp.concatenate([early_mine, early_other], 0)
    push_mine, push_other, early_words, late_mine, late_other = together(
        push_mine, push_other, early_words, late_mine, late_other
    )
    coefs = [
        jnp.concatenate([coef_real, jnp.ones((1,), jnp.float32)], 0),
        jnp.concatenate([coef_imag, jnp.zeros((1,), jnp.float32)], 0),
    ]
    tiles = operator_tiles(jnp.concatenate([couple, hamilton[None]], 0))
    total_rows = side_size * slot_count
    damping = jnp.sum(pick_rates(deep_bath, gamma), 1)
    part_damping = jnp.sum(pick_rates(part_of(shallow_bath), gamma), 1)[:, None, None, None]
    part_own = part_damping * part_of(shallow_trial)
    sources = [held[k] for k in range(side_size)]
    near_sources, far_sources = sources[: side_size // 2], sources[side_size // 2 :]
    own, keep, send = push(deep_trial, push_mine, damping, tiles, total_rows, own=True)
    got = swap(send, 1)
    early_words, own = together(early_words, own)
    early_pull = pull(2 * deep_count, early_words, coefs, tiles, near_sources)
    early = keep + got
    first_far = held[side_size // 2]
    top_tables = []
    for distance in range(1, side_size):
        tied, _ = together(table, first_far) if distance >= side_size // 2 else (table, None)
        top_tables.append(swap(tied, distance))
    own_words = pack(first_row + places, places, bath_count, bath_count, places >= 0)
    part_words = jnp.concatenate(
        [own_words, part_mine, part_other, raised_of(table, 0)]
        + [raised_of(x, 1 + k) for k, x in enumerate(top_tables)],
        0,
    )
    push_other, early, early_pull, part_words, *sources = together(
        push_other, early, early_pull, part_words, *sources
    )
    near_sources, far_sources = sources[: side_size // 2], sources[side_size // 2 :]
    keep, send = push(theirs, push_other, damping, tiles, total_rows)
    part_words, send = together(part_words, send)
    got = swap(send, 1)
    parts = pull(2 * per_row, part_words, coefs, tiles, sources)
    got, parts = together(got, parts)
    part = swap(parts[per_row:], side_size)
    part = parts[:per_row] - part_own + part

    step_rows = per_row // finer if per_row % finer == 0 else per_row
    starts = list(range(0, slot_count, step_rows))
    plane = {start: start // per_row for start in starts}
    depth = {start: min(plane[start], row_count - 1 - plane[start]) for start in starts}
    order = sorted(starts, key=lambda start: (-depth[start], start))
    middle = side_size // 4

    def blocks_of(start, low, high):
        def piece(x, block):
            begin = block * slot_count + start
            return x[begin : begin + step_rows]

        return [piece(early, b) + piece(keep, b) + piece(got, b) for b in range(low, high)]

    def launch(start):
        blocks = blocks_of(start, middle, 2 * middle)
        return [swap(x, 2) for x in blocks]

    stages = line_stages(row_count, row)
    first = {q: launch(order[q]) for q in range(len(order))}
    kept = [
        early[b * slot_count : (b + 1) * slot_count]
        + keep[b * slot_count : (b + 1) * slot_count]
        + got[b * slot_count : (b + 1) * slot_count]
        for b in range(middle)
    ]
    late_other, *kept = together(late_other, *kept)
    away = pull(
        deep_count, late_other, coefs, tiles, far_sources, early_pull, deep_count
    )
    late_mine, away = together(late_mine, away)
    away = swap(away, side_size)
    deep_slope = pull(deep_count, late_mine, coefs, tiles, far_sources, early_pull, 0)
    own, deep_slope = together(own, deep_slope)
    value, coming, last = {}, {}, None
    for turn in range(len(order) + len(stages)):
        for stage in range(-1, len(stages)):
            q = turn - stage - 1
            if not 0 <= q < len(order):
                continue
            came = first[q] if stage < 0 else [coming[q]]
            if last is None:
                deep_slope, *came = together(deep_slope, *came)
            else:
                value[last], *came = together(value[last], *came)
            start = order[q]
            if stage < 0:
                blocks = [x[start : start + step_rows] + b for x, b in zip(kept, came)]
                for bit in range(2, bits):
                    size = len(blocks) // 2
                    blocks = [blocks[b] + swap(blocks[size + b], 1 << bit) for b in range(size)]
                value[q] = blocks[0]
            else:
                value[q] = stages[stage][1](value[q], came[0])
            if depth[start] == stage + 1:
                begin = start % per_row
                mine = part[begin : begin + step_rows]
                value[q] = value[q] + jnp.where(row == plane[start], mine, 0.0)
            if stage + 1 < len(stages):
                coming[q] = stages[stage + 1][0](value[q])
            last = q
    chunks = [value[order.index(start)] for start in starts]
    deep_slope = own + deep_slope + away
    shallow_slope = jnp.concatenate(chunks, 0)
    return (shallow_slope, deep_slope)


def solution(mesh):
    placed = (
        P("col", None, None, None),
        P("col", None, None, None),
        P(("row", "col"), None, None, None),
        P(("row", "col"), None, None, None),
        P(),
        P(),
        P(),
        P(),
        P(),
        P("col", None),
        P("col", None),
        P(("row", "col"), None),
        P(("row", "col"), None),
    )
    return jax.shard_map(
        section,
        mesh=mesh,
        in_specs=placed,
        out_specs=(P("col", None, None, None), P(("row", "col"), None, None, None)),
        check_vma=False,
    )
```
